32 devices in a mesh: dp: 8 (over y, x, core), mp: 4 (over z).
Axes of the slice: x: 2, y: 2, z: 4, core: 2. Of those that a mesh axis runs over, the one named last changes fastest.
Arguments:
- vit_features: bfloat16 [32, 256, 1024], P('dp', 'mp'), may hold values from -6 to 6
- patch_counts: int32 [32], P('dp'), may hold values from 64 to 192
- text_counts: int32 [32], P('dp'), may hold values from 1 to 63
- tile_dest: int32 [32], P('dp'), may hold values from 0 to 7, as said below
- text_embeds: bfloat16 [32, 256, 4096], P('dp', 'mp'), may hold values from -6 to 6
- w_proj: bfloat16 [1024, 4096], replicated, may hold values from -0.1875 to 0.1875
- b_proj: float32 [4096], replicated, may hold values from -3 to 3
- norm_gain: float32 [1, 4096], replicated, may hold values from 0.1 to 1.9
- w_qkv: bfloat16 [1, 4096, 8, 512], P(None, 'dp', 'mp'), may hold values from -0.375 to 0.375
- w_out: bfloat16 [1, 8, 256, 4096], P(None, 'mp', None, 'dp'), may hold values from -0.125 to 0.125
Outputs:
- hidden_out: bfloat16 [32, 256, 4096], P('dp', 'mp')
The draws below stay inside these ranges and needn't reach their ends.
Inputs may be any that keep to these rules, and one draw needn't show every extreme that they name: `tile_dest`: each language-model rank receives exactly 4 tiles; one source rank sends at most 2 tiles to one language-model rank, and every source rank sends 2 to some rank.
All inputs are finite; a program needn't handle non-finite values.
Results may differ from the reference program's by a relative error of at most 0.01.
Values may be sent and summed in bfloat16 or wider, within the bound.
A program may use at most 128 MiB of HBM per device.

```python
import math
import jax
import jax.numpy as jnp
from jax import lax

D = 4096
VD = 1024
HS = 128
KVH = 8
GROUP = 2
LAYERS = 1
TILE = 256
IMG_DEV = 4
IMAGES = 32
N_DP = 8
N_MP = 4


def draw_tile_dest(key, part):
    rank_total = IMAGES // IMG_DEV
    owner_key = jax.random.fold_in(key, 101)
    shift_key = jax.random.fold_in(key, 202)
    order_key = jax.random.fold_in(key, 303)
    owners = jax.random.permutation(owner_key, rank_total).astype(jnp.int32)
    offsets = (1 + jax.random.permutation(shift_key, rank_total - 1)).astype(jnp.int32)
    shifts = jnp.concatenate([jnp.zeros((1,), jnp.int32), offsets[:IMG_DEV - 2], jnp.zeros((1,), jnp.int32)])
    scores = jax.random.randint(order_key, (rank_total, IMG_DEV), 0, 1 << 20) * IMG_DEV + jnp.arange(IMG_DEV, dtype=jnp.int32)[None, :]
    layers = jnp.argsort(scores, axis=1)
    picked = jnp.take(shifts, layers)
    sources = jnp.arange(rank_total, dtype=jnp.int32)[:, None]
    destinations = jnp.take(owners, (sources + picked) % rank_total)
    return destinations.reshape(IMAGES).astype(jnp.int32)


def draw_w_qkv(key, part):
    base_key = jax.random.fold_in(key, 404)
    width_all = (GROUP + 2) * HS
    base = jax.random.truncated_normal(base_key, -4.0, 4.0, (LAYERS, D, KVH, width_all), jnp.float32) * D ** (-0.5)
    return base.astype(jnp.bfloat16)


def set_ends(result, own_key, smallest, largest):
    spot = [jax.random.randint(jax.random.fold_in(own_key, axis), (), 0, length) for axis, length in enumerate(result.shape)]
    longest = result.shape.index(max(result.shape))
    neighbour = spot[:longest] + [(spot[longest] + 1) % result.shape[longest]] + spot[longest + 1:]
    return result.at[tuple(spot)].set(smallest).at[tuple(neighbour)].set(largest)


def levels(rng, shape, cuts, smallest, top_value):
    factor_of, own = 1.0, jax.random.fold_in(rng, 6)
    for axis_at, parts in cuts:
        draws = jnp.exp(jax.random.uniform(jax.random.fold_in(own, axis_at), (parts,), jnp.float32, smallest / len(cuts), top_value / len(cuts)))
        factor_of = factor_of * jnp.repeat(draws, shape[axis_at] // parts).reshape([-1 if axis == axis_at else 1 for axis in range(len(shape))])
    return factor_of


def noise(rng, extent, width, bound, cuts=(), kind=jnp.bfloat16):
    array = jax.random.normal(rng, extent, jnp.float32) * width
    if len(cuts) > 0:
        array = levels(rng, extent, cuts, -0.22, 0.18) * array
    return jnp.clip(array, min=-bound, max=bound).astype(kind)


def setup_inputs(seed: int = 0) -> dict:
    keys = jax.random.split(jax.random.key(seed), 11)
    return {
        "vit_features": noise(keys[0], (IMAGES, TILE, VD), 1.0, 6.0, ((0, 8), (1, 4))),
        "patch_counts": set_ends(jax.random.randint(keys[1], (IMAGES,), TILE // 4, 3 * TILE // 4 + 1), jax.random.fold_in(keys[1], 1), TILE // 4, (3 * TILE // 4 + 1) - 1).astype(jnp.int32),
        "text_counts": set_ends(jax.random.randint(keys[2], (IMAGES,), 1, TILE // 4), jax.random.fold_in(keys[2], 1), 1, (TILE // 4) - 1).astype(jnp.int32),
        "tile_dest": draw_tile_dest(jax.random.fold_in(keys[10], 71), 0),
        "text_embeds": noise(keys[4], (IMAGES, TILE, D), 1.0, 6.0, ((0, 8), (1, 4))),
        "w_proj": noise(keys[5], (VD, D), VD ** -0.5, 0.1875),
        "b_proj": noise(keys[6], (D,), 0.5, 3.0, (), jnp.float32),
        "norm_gain": jnp.clip(1.0 + 0.18 * jax.random.normal(keys[7], (LAYERS, D), jnp.float32), 0.1, 1.9),
        "w_qkv": draw_w_qkv(jax.random.fold_in(keys[10], 71), 0),
        "w_out": noise(keys[9], (LAYERS, KVH, GROUP * HS, D), (KVH * GROUP * HS) ** -0.5, 0.125, ((1, 4), (3, 8))),
    }


rope_base = 500000.0
epsilon = 1e-05

def tile_angles(tile_size, head_size):
    half_size = head_size // 2
    inverse = jnp.exp(-(2.0 * jnp.arange(half_size, dtype=jnp.float32) / head_size) * math.log(rope_base))
    positions = jnp.arange(tile_size, dtype=jnp.float32)
    return positions[:, None] * inverse[None, :]

def rotate_half(values, angles):
    half_size = values.shape[-1] // 2
    cosine = jnp.cos(angles)
    sine_part = jnp.sin(angles)
    first_half = values[..., :half_size]
    second = values[..., half_size:]
    return jnp.concatenate([first_half * cosine - second * sine_part, second * cosine + first_half * sine_part], axis=-1)

def attend_tile(operands):
    tile_queries, tile_keys, tile_values, length = operands
    score_scale = 1.0 / math.sqrt(HS)
    scores = jnp.einsum('rhge,che->hgrc', tile_queries.astype(jnp.float32), tile_keys.astype(jnp.float32)) * score_scale
    row_ids = jnp.arange(TILE, dtype=jnp.int32)[:, None]
    col_ids = jnp.arange(TILE, dtype=jnp.int32)[None, :]
    allowed = (col_ids <= row_ids) & (col_ids < length)
    scores = jnp.where(allowed, scores, -1e+30)
    row_max = lax.optimization_barrier(jnp.max(scores, axis=-1, keepdims=True))
    weights = jnp.where(allowed, jnp.exp(scores - row_max), 0.0)
    probabilities = (weights / lax.optimization_barrier(jnp.sum(weights, axis=-1, keepdims=True))).astype(jnp.bfloat16)
    return jnp.einsum('hgrc,che->rhge', probabilities.astype(jnp.float32), tile_values.astype(jnp.float32)).astype(jnp.bfloat16)

def decoder_attention(hidden, gain_row, weights_qkv, weights_out, lengths, angles):
    image_total = hidden.shape[0]
    as_float = hidden.astype(jnp.float32)
    mean_square = lax.optimization_barrier(jnp.mean(as_float * as_float, axis=-1, keepdims=True))
    normed = (as_float * lax.rsqrt(mean_square + epsilon) * gain_row).astype(jnp.bfloat16)
    joined_rows = jnp.dot(normed.reshape(image_total * TILE, D), weights_qkv.reshape(D, KVH * (GROUP + 2) * HS), preferred_element_type=jnp.float32)
    joined_rows = joined_rows.reshape(image_total, TILE, KVH, GROUP + 2, HS)
    queries = rotate_half(joined_rows[:, :, :, :GROUP, :], angles[None, :, None, None, :]).astype(jnp.bfloat16)
    key_heads = rotate_half(joined_rows[:, :, :, GROUP, :], angles[None, :, None, :]).astype(jnp.bfloat16)
    value_heads = joined_rows[:, :, :, GROUP + 1, :].astype(jnp.bfloat16)
    attended = lax.map(attend_tile, (queries, key_heads, value_heads, lengths))
    attended = attended.reshape(image_total * TILE, KVH * GROUP * HS)
    out_rows = weights_out.reshape(KVH * GROUP * HS, D)
    shard_width = KVH // N_MP * GROUP * HS
    summed = jnp.zeros((image_total * TILE, D), jnp.float32)
    for shard_idx in range(N_MP):
        partial_sum = jnp.dot(attended[:, shard_idx * shard_width:(shard_idx + 1) * shard_width], out_rows[shard_idx * shard_width:(shard_idx + 1) * shard_width], preferred_element_type=jnp.float32)
        summed = summed + lax.optimization_barrier(partial_sum.astype(jnp.bfloat16)).astype(jnp.float32)
    return (as_float + summed.reshape(image_total, TILE, D)).astype(jnp.bfloat16)

def reference(vit_features, patch_counts, text_counts, tile_dest, text_embeds, w_proj, b_proj, norm_gain, w_qkv, w_out):
    image_total = tile_dest.shape[0]
    dest_ids = jnp.arange(N_DP, dtype=jnp.int32)
    dest_hot = (tile_dest[:, None] == dest_ids[None, :]).astype(jnp.int32)
    earlier = jnp.cumsum(dest_hot, axis=0) - dest_hot
    slot_ids = lax.optimization_barrier(jnp.sum(earlier * dest_hot, axis=1)).astype(jnp.int32)
    targets = (tile_dest * IMG_DEV + slot_ids).astype(jnp.int32)
    sources = jnp.zeros((image_total,), jnp.int32).at[targets].set(jnp.arange(image_total, dtype=jnp.int32))
    placed = jnp.take(vit_features, sources, axis=0)
    projected = jnp.dot(placed.reshape(image_total * TILE, VD), w_proj, preferred_element_type=jnp.float32) + b_proj
    projected = projected.reshape(image_total, TILE, D)
    row_ids = jnp.arange(TILE, dtype=jnp.int32)[None, :, None]
    image_end = patch_counts[:, None, None]
    text_end = (patch_counts + text_counts)[:, None, None]
    hidden = jnp.where(row_ids < image_end, projected, jnp.where(row_ids < text_end, text_embeds.astype(jnp.float32), 0.0)).astype(jnp.bfloat16)
    lengths = patch_counts + text_counts
    angles = tile_angles(TILE, HS)
    for layer_idx in range(LAYERS):
        hidden = decoder_attention(hidden, norm_gain[layer_idx], w_qkv[layer_idx], w_out[layer_idx], lengths, angles)
    return hidden
```

```python
import functools
import math

import jax
import jax.numpy as jnp
from jax import lax
from jax.experimental import pallas as pl
from jax.experimental.pallas import tpu as pltpu
from jax.sharding import PartitionSpec as P

HS = 128
GROUP = 2
CAP = 2
LANES = 128
VMEM_BYTES = 60 * 1024 * 1024


rope_base = 500000.0
epsilon = 1e-05


def tile_angles(tile_size, head_size):
    half_size = head_size // 2
    inverse = jnp.exp(
        -(2.0 * jnp.arange(half_size, dtype=jnp.float32) / head_size) * math.log(rope_base)
    )
    positions = jnp.arange(tile_size, dtype=jnp.float32)
    return positions[:, None] * inverse[None, :]


def exchange_tiles(vit_features, tile_dest, rank_count):
    image_count, local_rows, vision_width = vit_features.shape
    dest_ids = jnp.arange(rank_count, dtype=jnp.int32)
    own_hot = (tile_dest[:, None] == dest_ids[None, :]).astype(jnp.int32)
    own_before = jnp.sum((jnp.cumsum(own_hot, axis=0) - own_hot) * own_hot, axis=1)
    targets = tile_dest * CAP + own_before
    placing = (targets[:, None] == jnp.arange(rank_count * CAP, dtype=jnp.int32)[None, :]).astype(
        jnp.bfloat16
    )
    flat_rows = vit_features.reshape(image_count, local_rows * vision_width)
    flat_rows = jnp.concatenate(
        [flat_rows, jnp.ones((image_count, LANES), flat_rows.dtype)], axis=1
    )
    outgoing = jnp.dot(placing.T, flat_rows, preferred_element_type=jnp.float32).astype(
        jnp.bfloat16
    )
    outgoing = outgoing.reshape(rank_count, CAP, -1)
    incoming = lax.all_to_all(outgoing, "dp", split_axis=0, concat_axis=0, tiled=True)
    incoming = incoming.reshape(rank_count * CAP, -1)
    filled = incoming[:, local_rows * vision_width].astype(jnp.int32)
    place = jnp.cumsum(filled) - filled
    selector = (
        (place[None, :] == jnp.arange(image_count, dtype=jnp.int32)[:, None]) & (filled[None, :] > 0)
    ).astype(jnp.bfloat16)
    arrived = jnp.dot(
        selector,
        incoming[:, : local_rows * vision_width],
        preferred_element_type=jnp.float32,
    )
    return arrived.astype(jnp.bfloat16).reshape(image_count, local_rows, vision_width)


def line_gather(block, axis_name, first_needed, last_needed):
    count = lax.axis_size(axis_name)
    by_offset = {0: block}
    passing = block
    for hop in range(1, count):
        pairs = [
            (i, i + 1)
            for i in range(hop - 1, count - 1)
            if first_needed <= i - hop + 1 <= last_needed
        ]
        if not pairs:
            break
        passing = lax.ppermute(passing, axis_name, pairs)
        by_offset[count - hop] = passing
    passing = block
    for hop in range(1, count):
        pairs = [
            (i, i - 1)
            for i in range(1, count - hop + 1)
            if first_needed <= i + hop - 1 <= last_needed
        ]
        if not pairs:
            break
        passing = lax.ppermute(passing, axis_name, pairs)
        by_offset[hop] = by_offset[hop] + passing if hop in by_offset else passing
    return by_offset


def doubling_gather(block, axis_name, split_axis, settle=None):
    count = lax.axis_size(axis_name)
    bits = count.bit_length() - 1
    outer = list(range(1, bits))
    orders = (outer, outer[1:] + outer[:1])

    def send(array, bit):
        return lax.ppermute(array, axis_name, [(i, i ^ (1 << bit)) for i in range(count)])

    def half_of(array, half):
        size = array.shape[split_axis] // 2
        return lax.slice_in_dim(array, half * size, (half + 1) * size, axis=split_axis)

    whole = {0: block}
    for bit in outer:
        whole[1 << bit] = send(block, bit)
    if settle is not None:
        whole = settle(whole)
    parts = ({}, {})
    for mask in range(2, count, 2):
        if mask in whole:
            continue
        for half in (0, 1):
            parts[half][mask] = None
    for half in (0, 1):
        reached = [0]
        for bit in orders[half]:
            for base in list(reached):
                mask = base | (1 << bit)
                reached.append(mask)
                if mask in whole:
                    continue
                origin = half_of(whole[base], half) if base in whole else parts[half][base]
                parts[half][mask] = send(origin, bit)
    pieces = [(mask, None, array) for mask, array in whole.items()]
    for half in (0, 1):
        pieces += [(mask, half, array) for mask, array in parts[half].items()]
    if bits > 0:
        pieces += [(mask | 1, half, send(array, 0)) for mask, half, array in pieces]
    return pieces


def attend_kernel(
    keys,
    local_rows,
    patch_ref,
    length_ref,
    images_ref,
    text_ref,
    proj_ref,
    bias_ref,
    gain_ref,
    cos_ref,
    sin_ref,
    *rest,
):
    pieces = rest[: len(keys)]
    attended_ref, own_ref, hidden_s, normed_s, joined_s = rest[len(keys) :]
    tile = pl.program_id(0)
    patches = patch_ref[tile]
    length = length_ref[tile]
    tile_size, model_width = hidden_s.shape
    window = text_ref.shape[1]
    image_rows = tile_size - window
    chunk = 512
    row_ids = lax.broadcasted_iota(jnp.int32, (tile_size, 1), 0)
    squares = jnp.zeros((tile_size, 1), jnp.float32)
    for start in range(0, model_width, chunk):
        columns = slice(start, start + chunk)
        projected = (
            jnp.dot(
                images_ref[0, :image_rows],
                proj_ref[:, columns],
                preferred_element_type=jnp.float32,
            )
            + bias_ref[:, columns]
        )
        text = text_ref[0, :, columns].astype(jnp.float32)
        texts = jnp.concatenate([text] * (tile_size // window), axis=0)
        texts = jnp.where(row_ids < length, texts, 0.0)
        top = jnp.where(row_ids[:image_rows] < patches, projected, texts[:image_rows])
        rows = jnp.concatenate([top, texts[image_rows:]], axis=0).astype(jnp.bfloat16)
        hidden_s[:, columns] = rows
        rows = rows.astype(jnp.float32)
        squares = squares + jnp.sum(rows * rows, axis=1, keepdims=True)
    factor = lax.rsqrt(squares / model_width + epsilon)
    for start in range(0, model_width, chunk):
        columns = slice(start, start + chunk)
        normed_s[:, columns] = (
            hidden_s[:, columns].astype(jnp.float32) * factor * gain_ref[:, columns]
        ).astype(jnp.bfloat16)
    own_start = pl.multiple_of(lax.axis_index("mp") * local_rows, local_rows)
    own_ref[0] = hidden_s[pl.ds(own_start, local_rows), :]

    rank = lax.axis_index("dp")
    width = joined_s.shape[1]
    half_width = width // 2
    for side in (0, 1):
        total = None
        for (mask, half), piece in zip(keys, pieces):
            if half is not None and half != side:
                continue
            depth = piece.shape[0]
            start = pl.multiple_of((rank ^ mask) * depth, depth)
            block = piece[...] if half is not None else piece[:, side * half_width : (side + 1) * half_width]
            term = jnp.dot(
                normed_s[:, pl.ds(start, depth)], block, preferred_element_type=jnp.float32
            )
            total = term if total is None else total + term
        joined_s[:, side * half_width : (side + 1) * half_width] = total

    cosine = cos_ref[...]
    sine = sin_ref[...]

    def rotated(start):
        values = joined_s[:, start : start + HS]
        return (values * cosine + pltpu.roll(values, HS // 2, 1) * sine).astype(jnp.bfloat16)

    col_ids = lax.broadcasted_iota(jnp.int32, (1, tile_size), 1)
    allowed = (col_ids <= row_ids) & (col_ids < length)
    head_width = (GROUP + 2) * HS
    outputs = []
    for first in range(0, width, head_width):
        head_keys = rotated(first + GROUP * HS)
        values = joined_s[:, first + (GROUP + 1) * HS : first + head_width].astype(jnp.bfloat16)
        for group in range(GROUP):
            queries = rotated(first + group * HS)
            scores = lax.dot_general(
                queries, head_keys, (((1,), (1,)), ((), ())), preferred_element_type=jnp.float32
            ) * (1.0 / math.sqrt(HS))
            scores = jnp.where(allowed, scores, -1e30)
            row_max = jnp.max(scores, axis=1, keepdims=True)
            weights = jnp.where(allowed, jnp.exp(scores - row_max), 0.0)
            weights = (weights / jnp.sum(weights, axis=1, keepdims=True)).astype(jnp.bfloat16)
            outputs.append(
                jnp.dot(weights, values, preferred_element_type=jnp.float32).astype(jnp.bfloat16)
            )
    attended = jnp.concatenate(outputs, axis=1)
    for part in range(tile_size // local_rows):
        attended_ref[part, 0] = attended[part * local_rows : (part + 1) * local_rows]


def output_kernel(keys, attended_ref, own_ref, *rest):
    count = len(keys)
    pieces = rest[:count]
    out_ref = rest[count]
    buffers = rest[count + 1 : 2 * count + 1]
    joined_s, sems = rest[2 * count + 1 :]
    copies = [
        pltpu.make_async_copy(piece, buffer, sems.at[index])
        for index, (piece, buffer) in enumerate(zip(pieces, buffers))
    ]
    for copy in copies:
        copy.start()
    parts, _, depth = attended_ref.shape
    for part in range(parts):
        joined_s[:, part * depth : (part + 1) * depth] = attended_ref[part]
    rank = lax.axis_index("dp")
    masks = {}
    for index, (mask, half) in enumerate(keys):
        masks.setdefault(mask, []).append((index, half))
    for mask, members in masks.items():
        width = pieces[members[0][0]].shape[1]
        columns = pl.ds(pl.multiple_of((rank ^ mask) * width, width), width)
        total = None
        for index, half in members:
            copies[index].wait()
            rows = buffers[index].shape[0]
            start = 0 if half is None else half * rows
            term = jnp.dot(
                joined_s[:, start : start + rows],
                buffers[index][...],
                preferred_element_type=jnp.float32,
            )
            total = term if total is None else total + term
        out_ref[:, columns] = (own_ref[:, columns].astype(jnp.float32) + total).astype(jnp.bfloat16)


def body(
    vit_features,
    patch_counts,
    text_counts,
    tile_dest,
    text_embeds,
    w_proj,
    b_proj,
    norm_gain,
    w_qkv,
    w_out,
):
    rank_count = lax.axis_size("dp")
    mp_count = lax.axis_size("mp")
    mp_rank = lax.axis_index("mp")
    image_count, local_rows, vision_width = vit_features.shape
    tile_size = local_rows * mp_count
    model_width = w_proj.shape[1]
    window = tile_size // 4
    lengths = patch_counts + text_counts

    own_rows = (mp_rank * local_rows + jnp.arange(local_rows, dtype=jnp.int32))[None, :, None]
    in_text = (own_rows >= patch_counts[:, None, None]) & (own_rows < lengths[:, None, None])
    text_rows = jnp.where(in_text, text_embeds, jnp.zeros_like(text_embeds))
    spans = window // local_rows
    if spans > 1:
        text_rows = jnp.concatenate(
            [
                jnp.where(mp_rank % spans == part, text_rows, jnp.zeros_like(text_rows))
                for part in range(spans)
            ],
            axis=1,
        )
    vit_features, text_rows = lax.optimization_barrier((vit_features, text_rows))
    text_rows = lax.psum(text_rows, "mp")

    out_depth = w_out.shape[1] * w_out.shape[2]
    out_width = w_out.shape[3]
    out_local = w_out.reshape(out_depth, out_width)
    out_blocks = line_gather(out_local, "mp", 0, mp_count - 1)
    out_columns = jnp.zeros((mp_count, out_depth, out_width), out_local.dtype)
    for offset, block in out_blocks.items():
        out_columns = lax.dynamic_update_index_in_dim(
            out_columns, block, (mp_rank + offset) % mp_count, 0
        )
    out_columns = out_columns.reshape(mp_count * out_depth, out_width)

    arrived = exchange_tiles(vit_features, tile_dest, rank_count)
    qkv_local = w_qkv.reshape(w_qkv.shape[1], -1)
    qkv_width = qkv_local.shape[1]
    qkv_pieces = doubling_gather(qkv_local, "dp", 1)
    qkv_keys = [(mask, half) for mask, half, _ in qkv_pieces]
    qkv_arrays = [array for _, _, array in qkv_pieces]

    def settle(whole):
        nonlocal text_rows, arrived, qkv_arrays
        text_rows, arrived, qkv_arrays, whole = lax.optimization_barrier(
            (text_rows, arrived, qkv_arrays, whole)
        )
        return whole

    out_pieces = doubling_gather(out_columns, "dp", 0, settle)
    images = lax.all_gather(arrived, "mp", axis=1, tiled=True)

    images, out_arrays = lax.optimization_barrier((images, [array for _, _, array in out_pieces]))

    angles = tile_angles(tile_size, HS)
    cosine, sine = jnp.cos(angles), jnp.sin(angles)
    cosine = jnp.concatenate([cosine, cosine], axis=1)
    sine = jnp.concatenate([-sine, sine], axis=1)

    def fixed(array):
        return pl.BlockSpec(array.shape, lambda i: (0,) * array.ndim)

    bias = b_proj.reshape(1, -1)
    gain = norm_gain.reshape(1, -1)
    attended, own_hidden = pl.pallas_call(
        functools.partial(attend_kernel, qkv_keys, local_rows),
        grid=(image_count,),
        in_specs=[
            pl.BlockSpec(memory_space=pltpu.SMEM),
            pl.BlockSpec(memory_space=pltpu.SMEM),
            pl.BlockSpec((1, tile_size, vision_width), lambda i: (i, 0, 0)),
            pl.BlockSpec((1, window, model_width), lambda i: (i, 0, 0)),
            fixed(w_proj),
            fixed(bias),
            fixed(gain),
            fixed(cosine),
            fixed(sine),
        ]
        + [fixed(array) for array in qkv_arrays],
        out_specs=[
            pl.BlockSpec((mp_count, 1, local_rows, out_depth), lambda i: (0, i, 0, 0)),
            pl.BlockSpec((1, local_rows, model_width), lambda i: (i, 0, 0)),
        ],
        out_shape=[
            jax.ShapeDtypeStruct((mp_count, image_count, local_rows, out_depth), jnp.bfloat16),
            jax.ShapeDtypeStruct((image_count, local_rows, model_width), jnp.bfloat16),
        ],
        scratch_shapes=[
            pltpu.VMEM((tile_size, model_width), jnp.bfloat16),
            pltpu.VMEM((tile_size, model_width), jnp.bfloat16),
            pltpu.VMEM((tile_size, qkv_width), jnp.float32),
        ],
        compiler_params=pltpu.CompilerParams(vmem_limit_bytes=VMEM_BYTES),
        cost_estimate=pl.CostEstimate(
            flops=2 * image_count * tile_size * model_width * (vision_width + qkv_width),
            bytes_accessed=2 * model_width * (vision_width + qkv_width),
            transcendentals=0,
        ),
        name="attend",
    )(
        patch_counts, lengths, images, text_rows, w_proj, bias, gain, cosine, sine, *qkv_arrays
    )

    attended = lax.all_to_all(attended, "mp", split_axis=0, concat_axis=0, tiled=True)

    rows = image_count * local_rows
    out_keys = [(mask, half) for mask, half, _ in out_pieces]
    vmem = pl.BlockSpec(memory_space=pltpu.VMEM)
    result = pl.pallas_call(
        functools.partial(output_kernel, out_keys),
        in_specs=[vmem, vmem] + [pl.BlockSpec(memory_space=pl.ANY)] * len(out_arrays),
        out_specs=vmem,
        out_shape=jax.ShapeDtypeStruct((rows, model_width), jnp.bfloat16),
        scratch_shapes=[pltpu.VMEM(array.shape, array.dtype) for array in out_arrays]
        + [
            pltpu.VMEM((rows, mp_count * out_depth), jnp.bfloat16),
            pltpu.SemaphoreType.DMA((len(out_arrays),)),
        ],
        compiler_params=pltpu.CompilerParams(vmem_limit_bytes=VMEM_BYTES),
        cost_estimate=pl.CostEstimate(
            flops=2 * rows * model_width * mp_count * out_depth,
            bytes_accessed=2 * model_width * mp_count * out_depth,
            transcendentals=0,
        ),
        name="output",
    )(
        attended.reshape(mp_count, rows, out_depth),
        own_hidden.reshape(rows, model_width),
        *out_arrays,
    )
    return result.reshape(image_count, local_rows, model_width)


def solution(mesh):
    in_specs = (
        P("dp", "mp", None),
        P("dp"),
        P("dp"),
        P("dp"),
        P("dp", "mp", None),
        P(),
        P(),
        P(),
        P(None, "dp", "mp", None),
        P(None, "mp", None, "dp"),
    )
    out_specs = P("dp", "mp", None)
    return jax.shard_map(body, mesh=mesh, in_specs=in_specs, out_specs=out_specs, check_vma=False)
```
